32 devices in a mesh: ops: 8 (over z, y), site: 4 (over x, core).
Axes of the slice: x: 2, y: 2, z: 4, core: 2. Of those that a mesh axis runs over, the one named last changes fastest.
Arguments:
- wavefunction: bfloat16 [2048, 2048], replicated, may hold values from -6 to 6
- left_blocks: bfloat16 [64, 16, 192, 192], P('ops', 'site'), may hold values from -0.4375 to 0.4375
- right_blocks: bfloat16 [64, 16, 192, 192], P('ops', 'site'), may hold values from -0.15625 to 0.15625
- left_sector: int32 [2048], replicated, may hold values from 0 to 15, as said below
- right_sector: int32 [2048], replicated, may hold values from 0 to 15, as said below
- term_count: int32 [8], P('ops'), may hold values from 1 to 8, as said below
- left_energy: float32 [2048], replicated, may hold values from -1 to 1
- right_energy: float32 [2048], replicated, may hold values from -1 to 1
- subspace: bfloat16 [2, 16, 192, 2048], P(None, 'site'), may hold values from -0.0078125 to 0.0078125
Outputs:
- sigma: bfloat16 [16, 192, 2048], P('site')
- projections: float32 [2], replicated
The draws below stay inside these ranges and needn't reach their ends.
Inputs may be any that keep to these rules, and one draw needn't show every extreme that they name: `left_sector`: sector ids never fall along the bond; each of the 16 sectors has 1 to 192 states and one has exactly 192. `right_sector`: sector ids never fall along the bond; each of the 16 sectors has 1 to 192 states and one has exactly 192. `term_count`: some group has all 8 slots live.
All inputs are finite; a program needn't handle non-finite values.
Results may differ from the reference program's by a relative error of at most 0.0045.
Values may be sent and summed in bfloat16 or wider, within the bound.
A program may use at most 192 MiB of HBM per device.

```python
import jax
import jax.numpy as jnp
from jax import lax

M = 2048
NB = 16
MAXB = 192
TERMS_DEV = 8
SUB = 2
TERMS = 64
N_OPS = 8


def draw_term_count(key, part):
    base_counts = jax.random.randint(jax.random.fold_in(key, 11), (N_OPS,), 1, TERMS_DEV // 2 + 1)
    fullest = jax.random.randint(jax.random.fold_in(key, 12), (), 0, N_OPS)
    return jnp.where(jnp.arange(N_OPS) == fullest, TERMS_DEV, base_counts).astype(jnp.int32)


def sector_draw(key):
    biggest = jax.random.randint(jax.random.fold_in(key, 1), (), 0, NB)
    remaining = jnp.int32(M - MAXB)
    sizes = []
    for label in range(NB):
        after = jnp.int32(NB - 1 - label) - (biggest > label).astype(jnp.int32)
        lower = jnp.maximum(1, remaining - after * MAXB)
        upper = jnp.minimum(MAXB, remaining - after)
        picked = jax.random.randint(jax.random.fold_in(key, 100 + label), (), lower, upper + 1)
        is_big = biggest == label
        size_now = jnp.where(is_big, jnp.int32(MAXB), picked).astype(jnp.int32)
        remaining = jnp.where(is_big, remaining, remaining - picked).astype(jnp.int32)
        sizes.append(size_now)
    ends = jnp.cumsum(jnp.stack(sizes)).astype(jnp.int32)
    positions = jnp.arange(M, dtype=jnp.int32)
    return jnp.sum((ends[None, :] <= positions[:, None]).astype(jnp.int32), axis=1).astype(jnp.int32)


def draw_left_sector(key, part):
    return sector_draw(jax.random.fold_in(key, 31))


def draw_right_sector(key, part):
    return sector_draw(jax.random.fold_in(key, 32))


def shard_levels(own_key, shape, shards, low, top_value):
    def one(axis_at, parts):
        heights = jax.random.uniform(jax.random.fold_in(jax.random.fold_in(own_key, 6), axis_at), (parts,), jnp.float32, low / len(shards), top_value / len(shards))
        return jnp.repeat(jnp.exp(heights), shape[axis_at] // parts).reshape((-1,) + (1,) * (len(shape) - axis_at - 1))

    loudness = one(*shards[0])
    for cut in shards[1:]:
        loudness = loudness * one(*cut)
    return loudness


def scatter_about(key, shape, deviation, reach, shards=(), held_as=jnp.bfloat16):
    drawn = deviation * jax.random.normal(key, shape, jnp.float32)
    if shards:
        drawn = drawn * shard_levels(key, shape, shards, -0.22, 0.18)
    return jnp.clip(drawn, -reach, reach).astype(held_as)


def setup_inputs(seed: int = 0) -> dict:
    seeds = jax.random.split(jax.random.key(seed), 10)
    wavefunction = scatter_about(seeds[0], (M, M), 1.0, 6.0)
    left_blocks = scatter_about(seeds[1], (TERMS, NB, MAXB, MAXB), MAXB ** -0.5, 0.4375, ((0, 8), (1, 4)))
    right_blocks = scatter_about(seeds[2], (TERMS, NB, MAXB, MAXB), (MAXB * TERMS_DEV * N_OPS // 8) ** -0.5, 0.15625, ((0, 8), (1, 4)))
    left_sector = draw_left_sector(jax.random.fold_in(seeds[9], 71), 0)
    right_sector = draw_right_sector(jax.random.fold_in(seeds[9], 71), 0)
    term_count = draw_term_count(jax.random.fold_in(seeds[9], 71), 0)
    left_energy = jnp.clip(jax.random.uniform(seeds[6], (M,), jnp.float32, -1.0, 1.0), -1.0, 1.0)
    right_energy = jnp.clip(jax.random.uniform(seeds[7], (M,), jnp.float32, -1.0, 1.0), -1.0, 1.0)
    subspace = scatter_about(seeds[8], (SUB, NB, MAXB, M), (1.0 / M), 0.0078125, ((1, 4),))
    return {"wavefunction": wavefunction, "left_blocks": left_blocks, "right_blocks": right_blocks, "left_sector": left_sector, "right_sector": right_sector, "term_count": term_count, "left_energy": left_energy, "right_energy": right_energy, "subspace": subspace}


def sector_tables(sector_ids, sectors):
    labels = jnp.arange(sectors, dtype=jnp.int32)
    sector_starts = jnp.sum((sector_ids[None, :] < labels[:, None]).astype(jnp.int32), axis=1)
    sector_sizes = jnp.sum((sector_ids[None, :] == labels[:, None]).astype(jnp.int32), axis=1)
    return sector_starts.astype(jnp.int32), sector_sizes.astype(jnp.int32)


def reference(wavefunction, left_blocks, right_blocks, left_sector, right_sector, term_count, left_energy, right_energy, subspace):
    left_start, left_size = sector_tables(left_sector, NB)
    right_start, right_size = sector_tables(right_sector, NB)
    positions = jnp.arange(MAXB, dtype=jnp.int32)
    left_inside = positions[None, :] < left_size[:, None]
    right_inside = positions[None, :] < right_size[:, None]
    left_masks = left_inside[:, :, None] & left_inside[:, None, :]
    right_masks = right_inside[:, :, None] & right_inside[:, None, :]
    psi_padded = jnp.concatenate([wavefunction, jnp.zeros((MAXB, M), wavefunction.dtype)], axis=0)
    psi_slabs = jax.vmap(lambda row_start: lax.dynamic_slice_in_dim(psi_padded, row_start, MAXB, 0))(left_start)
    slab_values = psi_slabs.astype(jnp.float32)
    row_count = NB * MAXB

    def term_product(accum, term_idx):
        live = (term_idx % TERMS_DEV) < term_count[term_idx // TERMS_DEV]

        def apply_term(summed_in):
            blocks = jnp.where(left_masks, left_blocks[term_idx], jnp.zeros((), left_blocks.dtype)).astype(jnp.float32)
            left_image = jnp.einsum("qab,qbc->qac", blocks, slab_values, precision=lax.Precision.HIGHEST)
            rounded = lax.optimization_barrier(left_image.astype(jnp.bfloat16)).astype(jnp.float32)
            rounded = rounded.reshape(row_count, M)
            padded_image = jnp.concatenate([rounded, jnp.zeros((row_count, MAXB), jnp.float32)], axis=1)
            right_terms = jnp.where(right_masks, right_blocks[term_idx], jnp.zeros((), right_blocks.dtype)).astype(jnp.float32)

            def one_sector(sector, summed):
                col_start = right_start[sector]
                window = lax.dynamic_slice_in_dim(padded_image, col_start, MAXB, 1)
                added = jnp.dot(window, right_terms[sector].T, precision=lax.Precision.HIGHEST)
                previous = lax.dynamic_slice_in_dim(summed, col_start, MAXB, 1)
                return lax.dynamic_update_slice_in_dim(summed, previous + added, col_start, 1)

            return lax.fori_loop(0, NB, one_sector, summed_in)

        return lax.cond(live, apply_term, lambda kept: kept, accum), None

    terms_padded, ignored = lax.scan(term_product, jnp.zeros((row_count, M + MAXB), jnp.float32), jnp.arange(TERMS_DEV * N_OPS, dtype=jnp.int32))
    terms = terms_padded[:, :M].reshape(NB, MAXB, M)
    psi_rows = jnp.where(left_inside[:, :, None], slab_values, jnp.float32(0.0))
    energy_padded = jnp.concatenate([left_energy, jnp.zeros((MAXB,), jnp.float32)])
    energy_rows = jax.vmap(lambda row_start: lax.dynamic_slice_in_dim(energy_padded, row_start, MAXB, 0))(left_start)
    sigma_full = terms + (energy_rows[:, :, None] + right_energy[None, None, :]) * psi_rows
    projections = jnp.sum(subspace.astype(jnp.float32) * sigma_full[None], axis=(1, 2, 3))
    return sigma_full.astype(jnp.bfloat16), projections
```

```python
import functools

import jax
import jax.numpy as jnp
from jax import lax
from jax.experimental import pallas as pl
from jax.experimental.pallas import tpu as pltpu
from jax.sharding import PartitionSpec as P

LANE = 128
MESH = pl.DeviceIdType.MESH
CHUNK = 256


def round_up(value, step):
    return (value + step - 1) // step * step


def step_kernel(
    groups, sites,
    tables, count, left_hbm, right_hbm, psi_hbm, vec_hbm, share_hbm, left_e_ref, right_e_ref,
    out_ref, corr_out,
    left, right, psi, vec, vec_share, slab, psi_share, e_share,
    rbuf, right_pad, psi_pad, images, terms, spread, placed, pick,
    part, pair_in, sending, outer_in, acc, corr_mine, corr_ops, corr_sites,
    load_s, pair_s, pair_r, x_s, x_r, xf_s, xf_r,
    y_s, y_r, outer_s, outer_r, gath_s, gath_r, fwd_s, fwd_r, ops_s, ops_r, site_s, site_r,
):
    half_slots, _, sec_dev, widest, _ = left.shape
    slots = 2 * half_slots
    rows = slab.shape[1]
    bond_dim = psi.shape[2]
    vectors = vec.shape[0]
    sectors = sec_dev * sites
    wide = psi_pad.shape[2]
    shift = wide - widest
    window = round_up(widest + LANE - 1, LANE)
    outer = groups // 2
    share = rows // groups
    chunks = bond_dim // CHUNK
    tiles = bond_dim // LANE
    half_sectors = sectors // 2
    half_cols = slots * widest // 2
    outside = -(-(bond_dim - CHUNK - 2 * (widest - 1)) // widest)
    overlap = min(sectors, sectors - outside)

    here = lax.axis_index("site")
    me = lax.axis_index("ops")
    xs = here // 2
    core = here % 2
    peer_site = xs * 2 + 1 - core
    across = (1 - xs) * 2 + core
    row = me // 2
    side = me % 2
    peer = row * 2 + 1 - side

    def sector_of(n):
        return jnp.where(xs == 0, n, sectors - 1 - n)

    def base_of(c):
        return pl.multiple_of(jnp.where(xs == 0, c * CHUNK, bond_dim - (c + 1) * CHUNK), CHUNK)

    def order_of(w):
        return jnp.where(xs == 0, here * sec_dev + w, sectors - 1 - here * sec_dev - w)

    def remote(src, dst, send_sem, recv_sem, target):
        return pltpu.make_async_remote_copy(
            src_ref=src, dst_ref=dst, send_sem=send_sem, recv_sem=recv_sem,
            device_id=target, device_id_type=MESH,
        )

    loads = [
        pltpu.make_async_copy(right_hbm, right, load_s.at[0]),
        pltpu.make_async_copy(left_hbm, left, load_s.at[1]),
        pltpu.make_async_copy(psi_hbm, psi, load_s.at[2]),
        pltpu.make_async_copy(share_hbm.at[:, me], vec_share, load_s.at[3]),
    ]
    for k in range(vectors):
        for t in range(tiles):
            loads.append(
                pltpu.make_async_copy(
                    vec_hbm.at[k, :, t * LANE : (t + 1) * LANE], vec.at[k, t],
                    load_s.at[4 + k * tiles + t],
                )
            )
    for load in loads:
        load.start()

    barrier = pltpu.get_barrier_semaphore()
    for k in range(1, groups):
        pl.semaphore_signal(
            barrier, inc=1, device_id={"ops": lax.rem(me + k, groups)}, device_id_type=MESH
        )
    for k in range(1, sites):
        pl.semaphore_signal(
            barrier, inc=1, device_id={"site": lax.rem(here + k, sites)}, device_id_type=MESH
        )

    lane_in = lax.broadcasted_iota(jnp.int32, (widest, wide), 0)
    lane_out = lax.broadcasted_iota(jnp.int32, (widest, wide), 1)
    lower = (lane_in == lane_out).astype(jnp.bfloat16)
    upper = (lane_in + shift == lane_out).astype(jnp.bfloat16)

    loads[0].wait()

    def pack(w, carry):
        n = order_of(w)
        for p in range(half_slots):
            even = jnp.dot(
                right[2 * p, w], lower, preferred_element_type=jnp.float32
            ).astype(jnp.bfloat16)
            odd = jnp.dot(
                right[2 * p + 1, w], upper, preferred_element_type=jnp.float32
            ).astype(jnp.bfloat16)
            at = 2 * p * widest
            rbuf[n, :, at : at + LANE] = even[:, :LANE]
            rbuf[n, :, at + LANE : at + 2 * LANE] = even[:, LANE:] + odd[:, :LANE]
            rbuf[n, :, at + 2 * LANE : at + 3 * LANE] = odd[:, LANE:]
        return carry

    lax.fori_loop(0, sec_dev, pack, 0)
    pl.semaphore_wait(barrier, groups - 1 + sites - 1)

    def to_pair(n):
        return remote(
            rbuf.at[n], rbuf.at[n], pair_s.at[n], pair_r.at[n], {"site": peer_site}
        )

    my_half = pl.ds(pl.multiple_of(core * half_cols, half_cols), half_cols)
    peer_half = pl.ds(pl.multiple_of((1 - core) * half_cols, half_cols), half_cols)

    def to_across(n):
        far_n = sectors - 1 - n
        return remote(
            rbuf.at[n, :, my_half], rbuf.at[far_n, :, my_half],
            x_s.at[n], x_r.at[far_n - half_sectors], {"site": across},
        )

    def forward(n, columns):
        return remote(
            rbuf.at[n, :, columns], rbuf.at[n, :, columns],
            xf_s.at[n - half_sectors], xf_r.at[n - half_sectors], {"site": peer_site},
        )

    def start_pair(w, carry):
        to_pair(order_of(w)).start()
        return carry

    lax.fori_loop(0, sec_dev, start_pair, 0)

    def start_across(idx, carry):
        n = half_sectors - 1 - idx
        owner = sector_of(n) // sec_dev

        @pl.when(owner != here)
        def _():
            to_pair(n).wait_recv()

        to_across(n).start()
        return carry

    lax.fori_loop(0, half_sectors, start_across, 0)

    first_sector = here * sec_dev

    span = window // LANE

    def window_of(start):
        first = jnp.minimum(start // LANE, tiles - span)
        return first, start - first * LANE

    right_pad[...] = jnp.zeros_like(right_pad)
    placed[...] = jnp.zeros_like(placed)
    acc[...] = jnp.zeros_like(acc)

    loads[1].wait()
    live_count = count[0]
    row_at = lax.broadcasted_iota(jnp.int32, (widest, widest), 0)
    for q in range(sec_dev):
        size_now = tables[1, first_sector + q]
        inside = row_at < size_now

        def mask(p, carry, q=q, inside=inside):
            for parity in range(2):
                keep = inside & (row_at * 0 + (2 * p + parity) < live_count)
                left[p, parity, q] = jnp.where(
                    keep, left[p, parity, q].astype(jnp.float32), 0.0
                ).astype(jnp.bfloat16)
            return carry

        lax.fori_loop(0, half_slots, mask, 0)

    loads[2].wait()
    for q in range(sec_dev):
        first, offset = window_of(tables[0, first_sector + q])
        out_row = lax.broadcasted_iota(jnp.int32, (widest, window), 0)
        in_row = lax.broadcasted_iota(jnp.int32, (widest, window), 1)
        size_now = tables[1, first_sector + q]
        choose = ((in_row == out_row + offset) & (out_row < size_now)).astype(jnp.bfloat16)
        found = jnp.dot(
            choose, jnp.concatenate([psi[first + t] for t in range(span)], axis=0),
            preferred_element_type=jnp.float32,
        ).astype(jnp.bfloat16)
        for t in range(tiles):
            slab[t, q * widest : (q + 1) * widest, :] = found[:, t * LANE : (t + 1) * LANE]

    share_at = me * share
    share_q = first_sector + share_at // widest
    share_off = share_at % widest
    first, offset = window_of(tables[0, share_q])
    out_row = lax.broadcasted_iota(jnp.int32, (share, window), 0) + share_off
    in_row = lax.broadcasted_iota(jnp.int32, (share, window), 1)
    share_mask = (in_row == out_row + offset) & (out_row < tables[1, share_q])
    choose = share_mask.astype(jnp.bfloat16)
    psi_share[...] = jnp.dot(
        choose, jnp.concatenate([psi[first + t] for t in range(span)], axis=0),
        preferred_element_type=jnp.float32,
    ).astype(jnp.bfloat16)
    energies = jnp.concatenate([left_e_ref[first + t] for t in range(span)], axis=1)
    e_share[...] = jnp.sum(jnp.where(share_mask, energies, 0.0), axis=1, keepdims=True)
    for load in loads[3:]:
        load.wait()

    def apply_sector(n):
        sector = sector_of(n)
        size_now = tables[3, sector]
        first, offset = window_of(tables[2, sector])
        place = lax.broadcasted_iota(jnp.int32, (window, wide), 0)
        column = lax.broadcasted_iota(jnp.int32, (window, wide), 1)
        at_low = ((place == column + offset) & (column < size_now)).astype(jnp.bfloat16)
        moved = column - shift
        at_high = (
            (place == moved + offset) & (moved >= 0) & (moved < size_now)
        ).astype(jnp.bfloat16)
        block = jnp.concatenate([slab[first + t] for t in range(span)], axis=1)
        psi_pad[0] = jnp.dot(block, at_low, preferred_element_type=jnp.float32).astype(jnp.bfloat16)
        psi_pad[1] = jnp.dot(block, at_high, preferred_element_type=jnp.float32).astype(
            jnp.bfloat16
        )
        right_pad[0:widest, :] = rbuf[n]
        for q in range(sec_dev):
            at = q * widest
            even, odd = (
                jnp.dot(
                    left[:, parity, q].reshape(half_slots * widest, widest),
                    psi_pad[parity, at : at + widest, :],
                    preferred_element_type=jnp.float32,
                ).astype(jnp.bfloat16)
                for parity in range(2)
            )
            for p in range(half_slots):
                within = slice(p * widest, (p + 1) * widest)
                base = 2 * p * widest
                images[at : at + widest, base : base + LANE] = even[within, :LANE]
                images[at : at + widest, base + LANE : base + 2 * LANE] = (
                    even[within, LANE:] + odd[within, :LANE]
                )
                images[at : at + widest, base + 2 * LANE : base + 3 * LANE] = odd[within, LANE:]
        terms[...] = lax.dot_general(
            images[...], right_pad[...], (((1,), (1,)), ((), ())),
            preferred_element_type=jnp.float32,
        )
        for k in range(vectors):
            block = jnp.concatenate([vec[k, first + t] for t in range(span)], axis=1)
            spread[k] = jnp.dot(
                block, at_low, preferred_element_type=jnp.float32
            ).astype(jnp.bfloat16)
        step = 32

        def fold(idx, totals):
            at = pl.multiple_of(idx * step, step)
            values = terms[pl.ds(at, step), :]
            placed[sector, pl.ds(at, step), :] = values.astype(jnp.bfloat16)
            new = []
            for k in range(vectors):
                product = spread[k, pl.ds(at, step), :].astype(jnp.float32) * values
                folded = sum(
                    product[r : r + 8, c : c + LANE]
                    for r in range(0, step, 8) for c in range(0, wide, LANE)
                )
                new.append(totals[k] + folded)
            return tuple(new)

        totals = lax.fori_loop(
            0, rows // step, fold, tuple(acc[k] for k in range(vectors)), unroll=4
        )
        for k in range(vectors):
            acc[k] = totals[k]

    def y_copy(c):
        return remote(
            part.at[c, :, 1 - side], pair_in.at[c], y_s.at[c], y_r.at[c], {"ops": peer}
        )

    def outer_copy(c, k, target):
        return remote(
            sending.at[c, k], outer_in.at[c, k], outer_s.at[c, k], outer_r.at[c, k],
            {"ops": target},
        )

    def cols_of(c):
        return pl.ds(base_of(c), CHUNK)

    def gath_copy(c, k, source, target):
        block = out_ref.at[source, :, cols_of(c)]
        return remote(block, block, gath_s.at[c, k], gath_r.at[c, k], {"ops": target})

    def fwd_copy(c, k, source):
        block = out_ref.at[source, :, cols_of(c)]
        return remote(block, block, fwd_s.at[c, k], fwd_r.at[c, k], {"ops": peer})

    def place_chunk(c):
        base = base_of(c)
        low = jnp.int32(0)
        for r in range(sectors):
            low = low + (tables[2, r] + tables[3, r] <= base).astype(jnp.int32)
        low = jnp.minimum(low, sectors - overlap)
        source = lax.broadcasted_iota(jnp.int32, (wide, CHUNK), 0)
        target = lax.broadcasted_iota(jnp.int32, (wide, CHUNK), 1)
        for m in range(overlap):
            moved = source + (tables[2, low + m] - base)
            pick[m * wide : (m + 1) * wide, :] = (
                (moved == target) & (source < tables[3, low + m])
            ).astype(jnp.bfloat16)
        found = jnp.concatenate([placed[low + m] for m in range(overlap)], axis=1)
        value = jnp.dot(found, pick[...], preferred_element_type=jnp.float32)
        part[c] = value.reshape(outer, 2, share, CHUNK).astype(jnp.bfloat16)
        y_copy(c).start()

    def add_pair(c):
        y_copy(c).wait_recv()
        for k in range(outer - 1):
            dest = lax.rem(row + k + 1, outer)
            sending[c, k] = (
                part[c, dest, side].astype(jnp.float32) + pair_in[c, dest].astype(jnp.float32)
            ).astype(jnp.bfloat16)
            outer_copy(c, k, dest * 2 + side).start()

    def finish(c):
        for k in range(outer - 1):
            outer_copy(c, k, peer).wait_recv()
        cols = cols_of(c)
        total = part[c, row, side].astype(jnp.float32) + pair_in[c, row].astype(jnp.float32)
        for k in range(outer - 1):
            total = total + outer_in[c, k].astype(jnp.float32)
        diagonal = (e_share[...] + right_e_ref[0:1, cols]) * psi_share[:, cols].astype(jnp.float32)
        out_ref[me, :, cols] = (total + diagonal).astype(jnp.bfloat16)
        for k in range(outer - 1):
            gath_copy(c, k, me, lax.rem(row + k + 1, outer) * 2 + side).start()
        fwd_copy(c, outer - 1, me).start()
        for k in range(vectors):
            product = vec_share[k, :, cols].astype(jnp.float32) * diagonal
            acc[k] += sum(
                product[r : r + 8, at : at + LANE]
                for r in range(0, share, 8) for at in range(0, CHUNK, LANE)
            )

    def pass_on(c):
        for k in range(outer - 1):
            source = lax.rem(row - k - 1 + outer, outer) * 2 + side
            gath_copy(c, k, source, peer).wait_recv()
            fwd_copy(c, k, source).start()

    def done(n):
        return jnp.maximum(bond_dim - widest * (sectors - 1 - n), 0) // CHUNK

    def slot(n, carry):
        @pl.when(n >= half_sectors)
        def _():
            remote(
                rbuf.at[n, :, my_half], rbuf.at[n, :, my_half],
                x_s.at[0], x_r.at[n - half_sectors], {"site": across},
            ).wait_recv()
            forward(n, my_half).start()
            forward(n, peer_half).wait_recv()

        apply_sector(n)

        @pl.when(done(n) > done(n - 1))
        def _():
            place_chunk(done(n) - 1)

        @pl.when((done(n - 1) > done(n - 2)) & (n >= 1))
        def _():
            add_pair(done(n - 1) - 1)

        @pl.when((done(n - 2) > done(n - 3)) & (n >= 2))
        def _():
            finish(done(n - 2) - 1)

        @pl.when((done(n - 3) > done(n - 4)) & (n >= 3))
        def _():
            pass_on(done(n - 3) - 1)

        return carry

    lax.fori_loop(0, sectors, slot, 0)

    def plan(n):
        now = max(bond_dim - widest * (sectors - 1 - n), 0) // CHUNK
        before = max(bond_dim - widest * (sectors - n), 0) // CHUNK
        return now - 1 if now > before else None

    last = sectors - 1
    for stage, n in (
        (add_pair, last), (finish, last - 1), (pass_on, last - 2), (finish, last),
    ):
        c = plan(n)
        if c is not None:
            stage(c)

    corr_mine[...] = acc[...]
    corr_copies = []
    for k in range(1, groups):
        copy = remote(
            corr_mine, corr_ops.at[k], ops_s.at[k], ops_r.at[k], {"ops": lax.rem(me + k, groups)}
        )
        copy.start()
        corr_copies.append(copy)
    corr_ops[0] = corr_mine[...]

    for n in (last - 1, last):
        c = plan(n)
        if c is not None:
            pass_on(c)

    for copy in corr_copies:
        copy.wait_recv()

    def corr_add(g, total):
        return total + corr_ops[lax.rem(me - g + groups, groups)]

    corr_sites[0] = lax.fori_loop(0, groups, corr_add, jnp.zeros(acc.shape, jnp.float32))
    site_copies = []
    for k in range(1, sites):
        copy = remote(
            corr_sites.at[0], corr_sites.at[k], site_s.at[k], site_r.at[k],
            {"site": lax.rem(here + k, sites)},
        )
        copy.start()
        site_copies.append(copy)

    def last_waits(c, carry):
        fwd_copy(c, outer - 1, peer).wait_recv()
        for k in range(outer - 1):
            source = lax.rem(row - k - 1 + outer, outer) * 2 + 1 - side
            fwd_copy(c, k, source).wait_recv()
        y_copy(c).wait_send()
        for k in range(outer - 1):
            outer_copy(c, k, peer).wait_send()
            gath_copy(c, k, me, peer).wait_send()
            fwd_copy(c, k, me).wait_send()
        fwd_copy(c, outer - 1, me).wait_send()
        return carry

    lax.fori_loop(0, chunks, last_waits, 0)

    for copy in site_copies:
        copy.wait_recv()

    def site_add(g, total):
        return total + corr_sites[lax.rem(here - g + sites, sites)]

    corr = lax.fori_loop(0, sites, site_add, jnp.zeros(acc.shape, jnp.float32))
    for k in range(vectors):
        corr_out[k] = jnp.sum(corr[k])

    def x_waits(n, carry):
        to_across(n).wait_send()
        forward(n + half_sectors, my_half).wait_send()
        return carry

    lax.fori_loop(0, half_sectors, x_waits, 0)

    def pair_waits(w, carry):
        to_pair(order_of(w)).wait_send()
        return carry

    lax.fori_loop(0, sec_dev, pair_waits, 0)
    for copy in corr_copies + site_copies:
        copy.wait_send()


def local(
    wavefunction,
    left_blocks,
    right_blocks,
    left_sector,
    right_sector,
    term_count,
    left_energy,
    right_energy,
    subspace,
):
    slots, sec_dev, widest = left_blocks.shape[0], left_blocks.shape[1], left_blocks.shape[2]
    bond_dim = wavefunction.shape[0]
    vectors = subspace.shape[0]
    rows = sec_dev * widest
    sites = lax.axis_size("site")
    groups = lax.axis_size("ops")
    sectors = sec_dev * sites
    wide = round_up(widest, 256)
    window = round_up(widest + LANE - 1, LANE)
    share = rows // groups
    outer = groups // 2
    chunks = bond_dim // CHUNK
    tiles = bond_dim // LANE
    half_sectors = sectors // 2
    outside = -(-(bond_dim - CHUNK - 2 * (widest - 1)) // widest)
    overlap = min(sectors, sectors - outside)

    assert sites == 4 and slots % 4 == 0 and 2 * (wide - widest) == LANE and wide == 2 * LANE

    labels = jnp.arange(sectors, dtype=jnp.int32)
    ids = jnp.stack([left_sector, right_sector])
    starts = jnp.sum((ids[:, None, :] < labels[None, :, None]).astype(jnp.int32), axis=2)
    sizes = jnp.sum((ids[:, None, :] == labels[None, :, None]).astype(jnp.int32), axis=2)
    tables = jnp.stack([starts, sizes], axis=1).reshape(4, sectors)

    vmem = pl.BlockSpec(memory_space=pltpu.VMEM)
    smem = pl.BlockSpec(memory_space=pltpu.SMEM)
    hbm = pl.BlockSpec(memory_space=pl.ANY)
    dma = pltpu.SemaphoreType.DMA
    bf16, f32 = jnp.bfloat16, jnp.float32
    sigma, corr = pl.pallas_call(
        functools.partial(step_kernel, groups, sites),
        out_shape=(
            jax.ShapeDtypeStruct((groups, share, bond_dim), bf16),
            jax.ShapeDtypeStruct((vectors,), f32),
        ),
        in_specs=[smem, smem, hbm, hbm, hbm, hbm, hbm, vmem, vmem],
        out_specs=(vmem, smem),
        scratch_shapes=[
            pltpu.VMEM((slots // 2, 2, sec_dev, widest, widest), bf16),
            pltpu.VMEM((slots, sec_dev, widest, widest), bf16),
            pltpu.VMEM((tiles, LANE, bond_dim), bf16),
            pltpu.VMEM((vectors, tiles, rows, LANE), bf16),
            pltpu.VMEM((vectors, share, bond_dim), bf16),
            pltpu.VMEM((tiles, rows, LANE), bf16),
            pltpu.VMEM((share, bond_dim), bf16),
            pltpu.VMEM((share, 1), f32),
            pltpu.VMEM((sectors, widest, slots * widest), bf16),
            pltpu.VMEM((wide, slots * widest), bf16),
            pltpu.VMEM((2, rows, wide), bf16),
            pltpu.VMEM((rows, slots * widest), bf16),
            pltpu.VMEM((rows, wide), f32),
            pltpu.VMEM((vectors, rows, wide), bf16),
            pltpu.VMEM((sectors, rows, wide), bf16),
            pltpu.VMEM((overlap * wide, CHUNK), bf16),
            pltpu.VMEM((chunks, outer, 2, share, CHUNK), bf16),
            pltpu.VMEM((chunks, outer, share, CHUNK), bf16),
            pltpu.VMEM((chunks, outer - 1, share, CHUNK), bf16),
            pltpu.VMEM((chunks, outer - 1, share, CHUNK), bf16),
            pltpu.VMEM((vectors, 8, LANE), f32),
            pltpu.VMEM((vectors, 8, LANE), f32),
            pltpu.VMEM((groups, vectors, 8, LANE), f32),
            pltpu.VMEM((sites, vectors, 8, LANE), f32),
            dma((4 + vectors * tiles,)),
            dma((half_sectors,)), dma((half_sectors,)),
            dma((half_sectors,)), dma((half_sectors,)),
            dma((half_sectors,)), dma((half_sectors,)),
            dma((chunks,)), dma((chunks,)),
            dma((chunks, outer)), dma((chunks, outer)),
            dma((chunks, outer)), dma((chunks, outer)),
            dma((chunks, outer)), dma((chunks, outer)),
            dma((groups,)), dma((groups,)),
            dma((sites,)), dma((sites,)),
        ],
        compiler_params=pltpu.CompilerParams(
            collective_id=0, has_side_effects=True, vmem_limit_bytes=66_900_000
        ),
        name="davidson_step",
    )(
        tables,
        term_count,
        left_blocks.reshape(slots // 2, 2, sec_dev, widest, widest),
        right_blocks,
        wavefunction.reshape(tiles, LANE, bond_dim),
        subspace.reshape(vectors, rows, bond_dim),
        subspace.reshape(vectors, groups, share, bond_dim),
        left_energy.reshape(tiles, 1, LANE),
        right_energy[None, :],
    )
    return (sigma.reshape(sec_dev, widest, bond_dim), corr)


def solution(mesh):
    in_specs = (
        P(),
        P("ops", "site", None, None),
        P("ops", "site", None, None),
        P(),
        P(),
        P("ops"),
        P(),
        P(),
        P(None, "site", None, None),
    )
    out_specs = (P("site", None, None), P())
    return jax.shard_map(local, mesh=mesh, in_specs=in_specs, out_specs=out_specs, check_vma=False)
```

```python
import functools

import jax
import jax.numpy as jnp
from jax import lax
from jax.experimental import pallas as pl
from jax.experimental.pallas import tpu as pltpu
from jax.sharding import PartitionSpec as P

LANE = 128
MESH = pl.DeviceIdType.MESH
CHUNK = 256


def round_up(value, step):
    return (value + step - 1) // step * step


def step_kernel(
    groups, sites,
    tables, count, left_hbm, right_hbm, psi_hbm, vec_hbm, share_hbm, left_e_ref, right_e_ref,
    out_ref, corr_out,
    left, right, psi, vec, vec_share, slab, psi_share, e_share,
    rbuf, right_pad, psi_pad, images, terms, spread, placed, pick,
    part, pair_in, sending, outer_in, acc, corr_mine, corr_ops, corr_sites,
    load_s, pair_s, pair_r, x_s, x_r, xf_s, xf_r,
    y_s, y_r, outer_s, outer_r, gath_s, gath_r, fwd_s, fwd_r, ops_s, ops_r, site_s, site_r,
):
    half_slots, _, sec_dev, widest, _ = left.shape
    slots = 2 * half_slots
    vectors, halves, tiles, rows, _ = vec.shape
    bond_dim = psi.shape[2]
    sec_half = sec_dev // halves
    sectors = sec_dev * sites
    wide = psi_pad.shape[2]
    shift = wide - widest
    window = round_up(widest + LANE - 1, LANE)
    outer = groups // 2
    share = rows // groups
    items = bond_dim // CHUNK * halves
    half_sectors = sectors // 2
    half_cols = slots * widest // 2
    outside = -(-(bond_dim - CHUNK - 2 * (widest - 1)) // widest)
    overlap = min(sectors, sectors - outside)

    here = lax.axis_index("site")
    me = lax.axis_index("ops")
    xs = here // 2
    core = here % 2
    peer_site = xs * 2 + 1 - core
    across = (1 - xs) * 2 + core
    row = me // 2
    side = me % 2
    peer = row * 2 + 1 - side

    def sector_of(n):
        return jnp.where(xs == 0, n, sectors - 1 - n)

    def base_of(c):
        return pl.multiple_of(jnp.where(xs == 0, c * CHUNK, bond_dim - (c + 1) * CHUNK), CHUNK)

    def order_of(w):
        return jnp.where(xs == 0, here * sec_dev + w, sectors - 1 - here * sec_dev - w)

    def remote(src, dst, send_sem, recv_sem, target):
        return pltpu.make_async_remote_copy(
            src_ref=src, dst_ref=dst, send_sem=send_sem, recv_sem=recv_sem,
            device_id=target, device_id_type=MESH,
        )

    loads = [
        pltpu.make_async_copy(right_hbm, right, load_s.at[0]),
        pltpu.make_async_copy(left_hbm, left, load_s.at[1]),
        pltpu.make_async_copy(psi_hbm, psi, load_s.at[2]),
        pltpu.make_async_copy(share_hbm.at[:, :, me], vec_share, load_s.at[3]),
    ]
    for k in range(vectors):
        for h in range(halves):
            for t in range(tiles):
                loads.append(
                    pltpu.make_async_copy(
                        vec_hbm.at[k, h, :, t * LANE : (t + 1) * LANE], vec.at[k, h, t],
                        load_s.at[4 + (k * halves + h) * tiles + t],
                    )
                )
    for load in loads:
        load.start()

    barrier = pltpu.get_barrier_semaphore()
    for k in range(1, groups):
        pl.semaphore_signal(
            barrier, inc=1, device_id={"ops": lax.rem(me + k, groups)}, device_id_type=MESH
        )
    for k in range(1, sites):
        pl.semaphore_signal(
            barrier, inc=1, device_id={"site": lax.rem(here + k, sites)}, device_id_type=MESH
        )

    lane_in = lax.broadcasted_iota(jnp.int32, (widest, wide), 0)
    lane_out = lax.broadcasted_iota(jnp.int32, (widest, wide), 1)
    lower = (lane_in == lane_out).astype(jnp.bfloat16)
    upper = (lane_in + shift == lane_out).astype(jnp.bfloat16)

    right_pad[widest:, :] = jnp.zeros((wide - widest, slots * widest), jnp.bfloat16)
    placed[...] = jnp.zeros_like(placed)
    acc[...] = jnp.zeros_like(acc)
    loads[0].wait()

    def pack(w, carry):
        n = order_of(w)
        for p in range(half_slots):
            even = jnp.dot(
                right[2 * p, w], lower, preferred_element_type=jnp.float32
            ).astype(jnp.bfloat16)
            odd = jnp.dot(
                right[2 * p + 1, w], upper, preferred_element_type=jnp.float32
            ).astype(jnp.bfloat16)
            at = 2 * p * widest
            rbuf[n, :, at : at + LANE] = even[:, :LANE]
            rbuf[n, :, at + LANE : at + 2 * LANE] = even[:, LANE:] + odd[:, :LANE]
            rbuf[n, :, at + 2 * LANE : at + 3 * LANE] = odd[:, LANE:]
        return carry

    lax.fori_loop(0, sec_dev, pack, 0)
    pl.semaphore_wait(barrier, groups - 1 + sites - 1)

    def to_pair(n):
        return remote(
            rbuf.at[n], rbuf.at[n], pair_s.at[n], pair_r.at[n], {"site": peer_site}
        )

    my_half = pl.ds(pl.multiple_of(core * half_cols, half_cols), half_cols)
    peer_half = pl.ds(pl.multiple_of((1 - core) * half_cols, half_cols), half_cols)

    def to_across(n):
        far_n = sectors - 1 - n
        return remote(
            rbuf.at[n, :, my_half], rbuf.at[far_n, :, my_half],
            x_s.at[n], x_r.at[far_n - half_sectors], {"site": across},
        )

    def forward(n, columns):
        return remote(
            rbuf.at[n, :, columns], rbuf.at[n, :, columns],
            xf_s.at[n - half_sectors], xf_r.at[n - half_sectors], {"site": peer_site},
        )

    def start_pair(w, carry):
        to_pair(order_of(w)).start()
        return carry

    lax.fori_loop(0, sec_dev, start_pair, 0)

    first_sector = here * sec_dev

    span = window // LANE

    def window_of(start):
        first = jnp.minimum(start // LANE, tiles - span)
        return first, start - first * LANE

    loads[1].wait()
    live_count = count[0]
    row_at = lax.broadcasted_iota(jnp.int32, (widest, widest), 0)
    for q in range(sec_dev):
        size_now = tables[1, first_sector + q]
        inside = row_at < size_now

        def mask(p, carry, q=q, inside=inside):
            for parity in range(2):
                keep = inside & (row_at * 0 + (2 * p + parity) < live_count)
                left[p, parity, q] = jnp.where(
                    keep, left[p, parity, q].astype(jnp.float32), 0.0
                ).astype(jnp.bfloat16)
            return carry

        lax.fori_loop(0, half_slots, mask, 0)

    loads[2].wait()
    for q in range(sec_dev):
        first, offset = window_of(tables[0, first_sector + q])
        out_row = lax.broadcasted_iota(jnp.int32, (widest, window), 0)
        in_row = lax.broadcasted_iota(jnp.int32, (widest, window), 1)
        size_now = tables[1, first_sector + q]
        choose = ((in_row == out_row + offset) & (out_row < size_now)).astype(jnp.bfloat16)
        found = jnp.dot(
            choose, jnp.concatenate([psi[first + t] for t in range(span)], axis=0),
            preferred_element_type=jnp.float32,
        ).astype(jnp.bfloat16)
        h, at = q // sec_half, q % sec_half * widest
        for t in range(tiles):
            slab[h, t, at : at + widest, :] = found[:, t * LANE : (t + 1) * LANE]

    for h in range(halves):
        share_at = h * rows + me * share
        share_q = first_sector + share_at // widest
        share_off = share_at % widest
        first, offset = window_of(tables[0, share_q])
        out_row = lax.broadcasted_iota(jnp.int32, (share, window), 0) + share_off
        in_row = lax.broadcasted_iota(jnp.int32, (share, window), 1)
        share_mask = (in_row == out_row + offset) & (out_row < tables[1, share_q])
        choose = share_mask.astype(jnp.bfloat16)
        psi_share[h] = jnp.dot(
            choose, jnp.concatenate([psi[first + t] for t in range(span)], axis=0),
            preferred_element_type=jnp.float32,
        ).astype(jnp.bfloat16)
        energies = jnp.concatenate([left_e_ref[first + t] for t in range(span)], axis=1)
        e_share[h] = jnp.sum(jnp.where(share_mask, energies, 0.0), axis=1, keepdims=True)
    for load in loads[3:]:
        load.wait()

    def start_across(idx, carry):
        n = half_sectors - 1 - idx
        owner = sector_of(n) // sec_dev

        @pl.when(owner != here)
        def _():
            to_pair(n).wait_recv()

        to_across(n).start()
        return carry

    lax.fori_loop(0, half_sectors, start_across, 0)


    def apply_sector(n, h):
        sector = sector_of(n)
        size_now = tables[3, sector]
        first, offset = window_of(tables[2, sector])
        place = lax.broadcasted_iota(jnp.int32, (window, wide), 0)
        column = lax.broadcasted_iota(jnp.int32, (window, wide), 1)
        at_low = ((place == column + offset) & (column < size_now)).astype(jnp.bfloat16)
        moved = column - shift
        at_high = (
            (place == moved + offset) & (moved >= 0) & (moved < size_now)
        ).astype(jnp.bfloat16)
        block = jnp.concatenate([slab[h, first + t] for t in range(span)], axis=1)
        psi_pad[0] = jnp.dot(block, at_low, preferred_element_type=jnp.float32).astype(jnp.bfloat16)
        psi_pad[1] = jnp.dot(block, at_high, preferred_element_type=jnp.float32).astype(
            jnp.bfloat16
        )
        right_pad[0:widest, :] = rbuf[n]
        for q in range(sec_half):
            at = q * widest
            even, odd = (
                jnp.dot(
                    left[:, parity, h * sec_half + q].reshape(half_slots * widest, widest),
                    psi_pad[parity, at : at + widest, :],
                    preferred_element_type=jnp.float32,
                ).astype(jnp.bfloat16)
                for parity in range(2)
            )
            for p in range(half_slots):
                within = slice(p * widest, (p + 1) * widest)
                base = 2 * p * widest
                images[at : at + widest, base : base + LANE] = even[within, :LANE]
                images[at : at + widest, base + LANE : base + 2 * LANE] = (
                    even[within, LANE:] + odd[within, :LANE]
                )
                images[at : at + widest, base + 2 * LANE : base + 3 * LANE] = odd[within, LANE:]
        terms[...] = lax.dot_general(
            images[...], right_pad[...], (((1,), (1,)), ((), ())),
            preferred_element_type=jnp.float32,
        )
        for k in range(vectors):
            block = jnp.concatenate([vec[k, h, first + t] for t in range(span)], axis=1)
            spread[k] = jnp.dot(
                block, at_low, preferred_element_type=jnp.float32
            ).astype(jnp.bfloat16)
        step = 32

        def fold(idx, totals):
            at = pl.multiple_of(idx * step, step)
            values = terms[pl.ds(at, step), :]
            placed[h, sector, pl.ds(at, step), :] = values.astype(jnp.bfloat16)
            new = []
            for k in range(vectors):
                product = spread[k, pl.ds(at, step), :].astype(jnp.float32) * values
                folded = sum(
                    product[r : r + 8, c : c + LANE]
                    for r in range(0, step, 8) for c in range(0, wide, LANE)
                )
                new.append(totals[k] + folded)
            return tuple(new)

        totals = lax.fori_loop(
            0, rows // step, fold, tuple(acc[k] for k in range(vectors)), unroll=4
        )
        for k in range(vectors):
            acc[k] = totals[k]

    def y_copy(e):
        return remote(
            part.at[e, :, 1 - side], pair_in.at[e], y_s.at[e], y_r.at[e], {"ops": peer}
        )

    def outer_copy(e, k, target):
        return remote(
            sending.at[e, k], outer_in.at[e, k], outer_s.at[e, k], outer_r.at[e, k],
            {"ops": target},
        )

    def cols_of(e):
        return pl.ds(base_of(e // halves), CHUNK)

    def gath_copy(e, k, source, target):
        block = out_ref.at[e % halves, source, :, cols_of(e)]
        return remote(block, block, gath_s.at[e, k], gath_r.at[e, k], {"ops": target})

    def fwd_copy(e, k, source):
        block = out_ref.at[e % halves, source, :, cols_of(e)]
        return remote(block, block, fwd_s.at[e, k], fwd_r.at[e, k], {"ops": peer})

    def place_chunk(e):
        base = base_of(e // halves)
        low = jnp.int32(0)
        for r in range(sectors):
            low = low + (tables[2, r] + tables[3, r] <= base).astype(jnp.int32)
        low = jnp.minimum(low, sectors - overlap)
        source = lax.broadcasted_iota(jnp.int32, (wide, CHUNK), 0)
        target = lax.broadcasted_iota(jnp.int32, (wide, CHUNK), 1)
        for m in range(overlap):
            moved = source + (tables[2, low + m] - base)
            pick[m * wide : (m + 1) * wide, :] = (
                (moved == target) & (source < tables[3, low + m])
            ).astype(jnp.bfloat16)
        found = jnp.concatenate([placed[e % halves, low + m] for m in range(overlap)], axis=1)
        value = jnp.dot(found, pick[...], preferred_element_type=jnp.float32)
        part[e] = value.reshape(outer, 2, share, CHUNK).astype(jnp.bfloat16)
        y_copy(e).start()

    def add_pair(e):
        y_copy(e).wait_recv()
        for k in range(outer - 1):
            dest = lax.rem(row + k + 1, outer)
            sending[e, k] = (
                part[e, dest, side].astype(jnp.float32) + pair_in[e, dest].astype(jnp.float32)
            ).astype(jnp.bfloat16)
            outer_copy(e, k, dest * 2 + side).start()

    def diagonal_of(e):
        cols = cols_of(e)
        h = e % halves
        return (e_share[h] + right_e_ref[0:1, cols]) * psi_share[h, :, cols].astype(jnp.float32)

    def project_diagonal(e):
        diagonal = diagonal_of(e)
        for k in range(vectors):
            product = vec_share[k, e % halves, :, cols_of(e)].astype(jnp.float32) * diagonal
            acc[k] += sum(
                product[r : r + 8, at : at + LANE]
                for r in range(0, share, 8) for at in range(0, CHUNK, LANE)
            )

    def finish(e):
        for k in range(outer - 1):
            outer_copy(e, k, peer).wait_recv()
        total = part[e, row, side].astype(jnp.float32) + pair_in[e, row].astype(jnp.float32)
        for k in range(outer - 1):
            total = total + outer_in[e, k].astype(jnp.float32)
        out_ref[e % halves, me, :, cols_of(e)] = (total + diagonal_of(e)).astype(jnp.bfloat16)
        for k in range(outer - 1):
            gath_copy(e, k, me, lax.rem(row + k + 1, outer) * 2 + side).start()
        fwd_copy(e, outer - 1, me).start()

    def pass_on(e):
        for k in range(outer - 1):
            source = lax.rem(row - k - 1 + outer, outer) * 2 + side
            gath_copy(e, k, source, peer).wait_recv()
            fwd_copy(e, k, source).start()

    local_slots = half_sectors * halves
    slots_all = sectors * halves

    def slot_of(m):
        late = jnp.maximum(m - local_slots, 0)
        early = m < local_slots
        n = jnp.where(early, m % half_sectors, half_sectors + late // halves)
        return n, jnp.where(early, m // half_sectors, late % halves)

    def done(n):
        return jnp.maximum(bond_dim - widest * (sectors - 1 - n), 0) // CHUNK

    def run_stage(stage, m):
        n, h = slot_of(jnp.maximum(m, 0))

        @pl.when((m >= 0) & (m < slots_all) & (done(n) > done(n - 1)))
        def _():
            stage((done(n) - 1) * halves + h)

    stages = ((place_chunk, 0), (add_pair, 1), (finish, 3), (pass_on, 5))

    def slot(m, carry):
        n, h = slot_of(m)

        @pl.when((m >= local_slots) & (h == 0))
        def _():
            remote(
                rbuf.at[n, :, my_half], rbuf.at[n, :, my_half],
                x_s.at[0], x_r.at[n - half_sectors], {"site": across},
            ).wait_recv()
            forward(n, my_half).start()
            forward(n, peer_half).wait_recv()

        apply_sector(n, h)

        @pl.when((m >= local_slots) & (m < local_slots + items))
        def _():
            project_diagonal(m - local_slots)

        for stage, lag in stages:
            run_stage(stage, m - lag)

        return carry

    lax.fori_loop(0, slots_all, slot, 0)

    corr_mine[...] = acc[...]
    corr_copies = []
    for k in range(1, groups):
        copy = remote(
            corr_mine, corr_ops.at[k], ops_s.at[k], ops_r.at[k], {"ops": lax.rem(me + k, groups)}
        )
        copy.start()
        corr_copies.append(copy)
    corr_ops[0] = corr_mine[...]

    def drain(m, carry):
        for stage, lag in stages[1:]:
            run_stage(stage, m - lag)
        return carry

    lax.fori_loop(slots_all, slots_all + 1, drain, 0)

    for copy in corr_copies:
        copy.wait_recv()

    def corr_add(g, total):
        return total + corr_ops[lax.rem(me - g + groups, groups)]

    corr_sites[0] = lax.fori_loop(0, groups, corr_add, jnp.zeros(acc.shape, jnp.float32))
    site_copies = []
    for k in range(1, sites):
        copy = remote(
            corr_sites.at[0], corr_sites.at[k], site_s.at[k], site_r.at[k],
            {"site": lax.rem(here + k, sites)},
        )
        copy.start()
        site_copies.append(copy)

    lax.fori_loop(slots_all + 1, slots_all + 5, drain, 0)

    def last_waits(c, carry):
        fwd_copy(c, outer - 1, peer).wait_recv()
        for k in range(outer - 1):
            source = lax.rem(row - k - 1 + outer, outer) * 2 + 1 - side
            fwd_copy(c, k, source).wait_recv()
        y_copy(c).wait_send()
        for k in range(outer - 1):
            outer_copy(c, k, peer).wait_send()
            gath_copy(c, k, me, peer).wait_send()
            fwd_copy(c, k, me).wait_send()
        fwd_copy(c, outer - 1, me).wait_send()
        return carry

    lax.fori_loop(0, items, last_waits, 0)

    for copy in site_copies:
        copy.wait_recv()

    def site_add(g, total):
        return total + corr_sites[lax.rem(here - g + sites, sites)]

    corr = lax.fori_loop(0, sites, site_add, jnp.zeros(acc.shape, jnp.float32))
    for k in range(vectors):
        corr_out[k] = jnp.sum(corr[k])

    def x_waits(n, carry):
        to_across(n).wait_send()
        forward(n + half_sectors, my_half).wait_send()
        return carry

    lax.fori_loop(0, half_sectors, x_waits, 0)

    def pair_waits(w, carry):
        to_pair(order_of(w)).wait_send()
        return carry

    lax.fori_loop(0, sec_dev, pair_waits, 0)
    for copy in corr_copies + site_copies:
        copy.wait_send()


def local(
    wavefunction,
    left_blocks,
    right_blocks,
    left_sector,
    right_sector,
    term_count,
    left_energy,
    right_energy,
    subspace,
):
    slots, sec_dev, widest = left_blocks.shape[0], left_blocks.shape[1], left_blocks.shape[2]
    bond_dim = wavefunction.shape[0]
    vectors = subspace.shape[0]
    rows = sec_dev * widest
    sites = lax.axis_size("site")
    groups = lax.axis_size("ops")
    sectors = sec_dev * sites
    wide = round_up(widest, 256)
    window = round_up(widest + LANE - 1, LANE)
    outer = groups // 2
    halves = 2 if groups > 99 and rows // 2 % (16 * groups) == 0 and sec_dev % 2 == 0 else 1
    rows = rows // halves
    share = rows // groups
    items = bond_dim // CHUNK * halves
    tiles = bond_dim // LANE
    half_sectors = sectors // 2
    outside = -(-(bond_dim - CHUNK - 2 * (widest - 1)) // widest)
    overlap = min(sectors, sectors - outside)

    assert sites == 4 and slots % 4 == 0 and 2 * (wide - widest) == LANE and wide == 2 * LANE

    labels = jnp.arange(sectors, dtype=jnp.int32)
    ids = jnp.stack([left_sector, right_sector])
    starts = jnp.sum((ids[:, None, :] < labels[None, :, None]).astype(jnp.int32), axis=2)
    sizes = jnp.sum((ids[:, None, :] == labels[None, :, None]).astype(jnp.int32), axis=2)
    tables = jnp.stack([starts, sizes], axis=1).reshape(4, sectors)

    vmem = pl.BlockSpec(memory_space=pltpu.VMEM)
    smem = pl.BlockSpec(memory_space=pltpu.SMEM)
    hbm = pl.BlockSpec(memory_space=pl.ANY)
    dma = pltpu.SemaphoreType.DMA
    bf16, f32 = jnp.bfloat16, jnp.float32
    sigma, corr = pl.pallas_call(
        functools.partial(step_kernel, groups, sites),
        out_shape=(
            jax.ShapeDtypeStruct((halves, groups, share, bond_dim), bf16),
            jax.ShapeDtypeStruct((vectors,), f32),
        ),
        in_specs=[smem, smem, hbm, hbm, hbm, hbm, hbm, vmem, vmem],
        out_specs=(vmem, smem),
        scratch_shapes=[
            pltpu.VMEM((slots // 2, 2, sec_dev, widest, widest), bf16),
            pltpu.VMEM((slots, sec_dev, widest, widest), bf16),
            pltpu.VMEM((tiles, LANE, bond_dim), bf16),
            pltpu.VMEM((vectors, halves, tiles, rows, LANE), bf16),
            pltpu.VMEM((vectors, halves, share, bond_dim), bf16),
            pltpu.VMEM((halves, tiles, rows, LANE), bf16),
            pltpu.VMEM((halves, share, bond_dim), bf16),
            pltpu.VMEM((halves, share, 1), f32),
            pltpu.VMEM((sectors, widest, slots * widest), bf16),
            pltpu.VMEM((wide, slots * widest), bf16),
            pltpu.VMEM((2, rows, wide), bf16),
            pltpu.VMEM((rows, slots * widest), bf16),
            pltpu.VMEM((rows, wide), f32),
            pltpu.VMEM((vectors, rows, wide), bf16),
            pltpu.VMEM((halves, sectors, rows, wide), bf16),
            pltpu.VMEM((overlap * wide, CHUNK), bf16),
            pltpu.VMEM((items, outer, 2, share, CHUNK), bf16),
            pltpu.VMEM((items, outer, share, CHUNK), bf16),
            pltpu.VMEM((items, outer - 1, share, CHUNK), bf16),
            pltpu.VMEM((items, outer - 1, share, CHUNK), bf16),
            pltpu.VMEM((vectors, 8, LANE), f32),
            pltpu.VMEM((vectors, 8, LANE), f32),
            pltpu.VMEM((groups, vectors, 8, LANE), f32),
            pltpu.VMEM((sites, vectors, 8, LANE), f32),
            dma((4 + vectors * halves * tiles,)),
            dma((half_sectors,)), dma((half_sectors,)),
            dma((half_sectors,)), dma((half_sectors,)),
            dma((half_sectors,)), dma((half_sectors,)),
            dma((items,)), dma((items,)),
            dma((items, outer)), dma((items, outer)),
            dma((items, outer)), dma((items, outer)),
            dma((items, outer)), dma((items, outer)),
            dma((groups,)), dma((groups,)),
            dma((sites,)), dma((sites,)),
        ],
        compiler_params=pltpu.CompilerParams(
            collective_id=0, has_side_effects=True, vmem_limit_bytes=66_900_000
        ),
        name="davidson_step",
    )(
        tables,
        term_count,
        left_blocks.reshape(slots // 2, 2, sec_dev, widest, widest),
        right_blocks,
        wavefunction.reshape(tiles, LANE, bond_dim),
        subspace.reshape(vectors, halves, rows, bond_dim),
        subspace.reshape(vectors, halves, groups, share, bond_dim),
        left_energy.reshape(tiles, 1, LANE),
        right_energy[None, :],
    )
    return (sigma.reshape(sec_dev, widest, bond_dim), corr)


def solution(mesh):
    in_specs = (
        P(),
        P("ops", "site", None, None),
        P("ops", "site", None, None),
        P(),
        P(),
        P("ops"),
        P(),
        P(),
        P(None, "site", None, None),
    )
    out_specs = (P("site", None, None), P())
    return jax.shard_map(local, mesh=mesh, in_specs=in_specs, out_specs=out_specs, check_vma=False)
```

```python
import functools

import jax
import jax.numpy as jnp
from jax import lax
from jax.experimental import pallas as pl
from jax.experimental.pallas import tpu as pltpu
from jax.sharding import PartitionSpec as P

LANE = 128
MESH = pl.DeviceIdType.MESH
CHUNK = 256


def round_up(value, step):
    return (value + step - 1) // step * step


def step_kernel(
    groups, sites,
    tables, count, left_hbm, right_hbm, psi_hbm, vec_hbm, share_hbm, left_e_ref, right_e_ref,
    out_ref, corr_out,
    left, right, psi, vec, vec_share, slab, psi_share, e_share,
    rbuf, right_pad, psi_pad, images, terms, spread, placed, pick,
    part, pair_in, sending, outer_in, acc, corr_mine, corr_ops, corr_sites,
    load_s, pair_s, pair_r, x_s, x_r, xf_s, xf_r,
    y_s, y_r, outer_s, outer_r, gath_s, gath_r, fwd_s, fwd_r, ops_s, ops_r, site_s, site_r,
):
    half_slots, _, sec_dev, widest, _ = left.shape
    slots = 2 * half_slots
    vectors, halves, tiles, rows, _ = vec.shape
    bond_dim = psi.shape[2]
    sec_half = sec_dev // halves
    sectors = sec_dev * sites
    wide = psi_pad.shape[2]
    shift = wide - widest
    window = round_up(widest + LANE - 1, LANE)
    outer = groups // 2
    share = rows // groups
    items = bond_dim // CHUNK * halves
    half_sectors = sectors // 2
    half_cols = slots * widest // 2
    outside = -(-(bond_dim - CHUNK - 2 * (widest - 1)) // widest)
    overlap = min(sectors, sectors - outside)

    here = lax.axis_index("site")
    me = lax.axis_index("ops")
    xs = here // 2
    core = here % 2
    peer_site = xs * 2 + 1 - core
    across = (1 - xs) * 2 + core
    row = me // 2
    side = me % 2
    peer = row * 2 + 1 - side

    def sector_of(n):
        return jnp.where(xs == 0, n, sectors - 1 - n)

    def base_of(c):
        return pl.multiple_of(jnp.where(xs == 0, c * CHUNK, bond_dim - (c + 1) * CHUNK), CHUNK)

    def order_of(w):
        return jnp.where(xs == 0, here * sec_dev + w, sectors - 1 - here * sec_dev - w)

    def remote(src, dst, send_sem, recv_sem, target):
        return pltpu.make_async_remote_copy(
            src_ref=src, dst_ref=dst, send_sem=send_sem, recv_sem=recv_sem,
            device_id=target, device_id_type=MESH,
        )

    loads = [
        pltpu.make_async_copy(right_hbm, right, load_s.at[0]),
        pltpu.make_async_copy(left_hbm, left, load_s.at[1]),
        pltpu.make_async_copy(psi_hbm, psi, load_s.at[2]),
        pltpu.make_async_copy(share_hbm.at[:, :, me], vec_share, load_s.at[3]),
    ]
    for k in range(vectors):
        for h in range(halves):
            for t in range(tiles):
                loads.append(
                    pltpu.make_async_copy(
                        vec_hbm.at[k, h, :, t * LANE : (t + 1) * LANE], vec.at[k, h, t],
                        load_s.at[4 + (k * halves + h) * tiles + t],
                    )
                )
    for load in loads:
        load.start()

    barrier = pltpu.get_barrier_semaphore()
    for k in range(1, groups):
        pl.semaphore_signal(
            barrier, inc=1, device_id={"ops": lax.rem(me + k, groups)}, device_id_type=MESH
        )
    for k in range(1, sites):
        pl.semaphore_signal(
            barrier, inc=1, device_id={"site": lax.rem(here + k, sites)}, device_id_type=MESH
        )

    lane_in = lax.broadcasted_iota(jnp.int32, (widest, wide), 0)
    lane_out = lax.broadcasted_iota(jnp.int32, (widest, wide), 1)
    lower = (lane_in == lane_out).astype(jnp.bfloat16)
    upper = (lane_in + shift == lane_out).astype(jnp.bfloat16)

    right_pad[widest:, :] = jnp.zeros((wide - widest, slots * widest), jnp.bfloat16)
    placed[...] = jnp.zeros_like(placed)
    acc[...] = jnp.zeros_like(acc)
    loads[0].wait()

    def pack(w, carry):
        n = order_of(w)
        for p in range(half_slots):
            even = jnp.dot(
                right[2 * p, w], lower, preferred_element_type=jnp.float32
            ).astype(jnp.bfloat16)
            odd = jnp.dot(
                right[2 * p + 1, w], upper, preferred_element_type=jnp.float32
            ).astype(jnp.bfloat16)
            at = 2 * p * widest
            rbuf[n, :, at : at + LANE] = even[:, :LANE]
            rbuf[n, :, at + LANE : at + 2 * LANE] = even[:, LANE:] + odd[:, :LANE]
            rbuf[n, :, at + 2 * LANE : at + 3 * LANE] = odd[:, LANE:]
        return carry

    lax.fori_loop(0, sec_dev, pack, 0)
    pl.semaphore_wait(barrier, groups - 1 + sites - 1)

    def to_pair(n):
        return remote(
            rbuf.at[n], rbuf.at[n], pair_s.at[n], pair_r.at[n], {"site": peer_site}
        )

    my_half = pl.ds(pl.multiple_of(core * half_cols, half_cols), half_cols)
    peer_half = pl.ds(pl.multiple_of((1 - core) * half_cols, half_cols), half_cols)

    def to_across(n):
        far_n = sectors - 1 - n
        return remote(
            rbuf.at[n, :, my_half], rbuf.at[far_n, :, my_half],
            x_s.at[n], x_r.at[far_n - half_sectors], {"site": across},
        )

    def forward(n, columns):
        return remote(
            rbuf.at[n, :, columns], rbuf.at[n, :, columns],
            xf_s.at[n - half_sectors], xf_r.at[n - half_sectors], {"site": peer_site},
        )

    def start_pair(w, carry):
        to_pair(order_of(w)).start()
        return carry

    lax.fori_loop(0, sec_dev, start_pair, 0)

    first_sector = here * sec_dev

    span = window // LANE

    def window_of(start):
        first = jnp.minimum(start // LANE, tiles - span)
        return first, start - first * LANE

    loads[1].wait()
    live_count = count[0]
    row_at = lax.broadcasted_iota(jnp.int32, (widest, widest), 0)
    for q in range(sec_dev):
        size_now = tables[1, first_sector + q]
        inside = row_at < size_now

        def mask(p, carry, q=q, inside=inside):
            for parity in range(2):
                keep = inside & (row_at * 0 + (2 * p + parity) < live_count)
                left[p, parity, q] = jnp.where(
                    keep, left[p, parity, q].astype(jnp.float32), 0.0
                ).astype(jnp.bfloat16)
            return carry

        lax.fori_loop(0, half_slots, mask, 0)

    loads[2].wait()
    for q in range(sec_dev):
        first, offset = window_of(tables[0, first_sector + q])
        out_row = lax.broadcasted_iota(jnp.int32, (widest, window), 0)
        in_row = lax.broadcasted_iota(jnp.int32, (widest, window), 1)
        size_now = tables[1, first_sector + q]
        choose = ((in_row == out_row + offset) & (out_row < size_now)).astype(jnp.bfloat16)
        found = jnp.dot(
            choose, jnp.concatenate([psi[first + t] for t in range(span)], axis=0),
            preferred_element_type=jnp.float32,
        ).astype(jnp.bfloat16)
        h, at = q // sec_half, q % sec_half * widest
        for t in range(tiles):
            slab[h, t, at : at + widest, :] = found[:, t * LANE : (t + 1) * LANE]

    for h in range(halves):
        share_at = h * rows + me * share
        share_q = first_sector + share_at // widest
        share_off = share_at % widest
        first, offset = window_of(tables[0, share_q])
        out_row = lax.broadcasted_iota(jnp.int32, (share, window), 0) + share_off
        in_row = lax.broadcasted_iota(jnp.int32, (share, window), 1)
        share_mask = (in_row == out_row + offset) & (out_row < tables[1, share_q])
        choose = share_mask.astype(jnp.bfloat16)
        psi_share[h] = jnp.dot(
            choose, jnp.concatenate([psi[first + t] for t in range(span)], axis=0),
            preferred_element_type=jnp.float32,
        ).astype(jnp.bfloat16)
        energies = jnp.concatenate([left_e_ref[first + t] for t in range(span)], axis=1)
        e_share[h] = jnp.sum(jnp.where(share_mask, energies, 0.0), axis=1, keepdims=True)
    for load in loads[3:]:
        load.wait()

    def start_across(idx, carry):
        n = half_sectors - 1 - idx
        owner = sector_of(n) // sec_dev

        @pl.when(owner != here)
        def _():
            to_pair(n).wait_recv()

        to_across(n).start()
        return carry

    lax.fori_loop(0, half_sectors, start_across, 0)


    def apply_sector(n, h):
        sector = sector_of(n)
        size_now = tables[3, sector]
        first, offset = window_of(tables[2, sector])
        place = lax.broadcasted_iota(jnp.int32, (window, wide), 0)
        column = lax.broadcasted_iota(jnp.int32, (window, wide), 1)
        at_low = ((place == column + offset) & (column < size_now)).astype(jnp.bfloat16)
        moved = column - shift
        at_high = (
            (place == moved + offset) & (moved >= 0) & (moved < size_now)
        ).astype(jnp.bfloat16)
        block = jnp.concatenate([slab[h, first + t] for t in range(span)], axis=1)
        psi_pad[0] = jnp.dot(block, at_low, preferred_element_type=jnp.float32).astype(jnp.bfloat16)
        psi_pad[1] = jnp.dot(block, at_high, preferred_element_type=jnp.float32).astype(
            jnp.bfloat16
        )
        right_pad[0:widest, :] = rbuf[n]
        for q in range(sec_half):
            at = q * widest
            even, odd = (
                jnp.dot(
                    left[:, parity, h * sec_half + q].reshape(half_slots * widest, widest),
                    psi_pad[parity, at : at + widest, :],
                    preferred_element_type=jnp.float32,
                ).astype(jnp.bfloat16)
                for parity in range(2)
            )
            for p in range(half_slots):
                within = slice(p * widest, (p + 1) * widest)
                base = 2 * p * widest
                images[at : at + widest, base : base + LANE] = even[within, :LANE]
                images[at : at + widest, base + LANE : base + 2 * LANE] = (
                    even[within, LANE:] + odd[within, :LANE]
                )
                images[at : at + widest, base + 2 * LANE : base + 3 * LANE] = odd[within, LANE:]
        terms[...] = lax.dot_general(
            images[...], right_pad[...], (((1,), (1,)), ((), ())),
            preferred_element_type=jnp.float32,
        )
        for k in range(vectors):
            block = jnp.concatenate([vec[k, h, first + t] for t in range(span)], axis=1)
            spread[k] = jnp.dot(
                block, at_low, preferred_element_type=jnp.float32
            ).astype(jnp.bfloat16)
        step = 32

        def fold(idx, totals):
            at = pl.multiple_of(idx * step, step)
            values = terms[pl.ds(at, step), :]
            placed[h, sector, pl.ds(at, step), :] = values.astype(jnp.bfloat16)
            new = []
            for k in range(vectors):
                product = spread[k, pl.ds(at, step), :].astype(jnp.float32) * values
                folded = sum(
                    product[r : r + 8, c : c + LANE]
                    for r in range(0, step, 8) for c in range(0, wide, LANE)
                )
                new.append(totals[k] + folded)
            return tuple(new)

        totals = lax.fori_loop(
            0, rows // step, fold, tuple(acc[k] for k in range(vectors)), unroll=4
        )
        for k in range(vectors):
            acc[k] = totals[k]

    def y_copy(e):
        return remote(
            part.at[e, :, 1 - side], pair_in.at[e], y_s.at[e], y_r.at[e], {"ops": peer}
        )

    def outer_copy(e, k, target):
        return remote(
            sending.at[e, k], outer_in.at[e, k], outer_s.at[e, k], outer_r.at[e, k],
            {"ops": target},
        )

    def cols_of(e):
        return pl.ds(base_of(e // halves), CHUNK)

    def gath_copy(e, k, source, target):
        block = out_ref.at[e % halves, source, :, cols_of(e)]
        return remote(block, block, gath_s.at[e, k], gath_r.at[e, k], {"ops": target})

    def fwd_copy(e, k, source):
        block = out_ref.at[e % halves, source, :, cols_of(e)]
        return remote(block, block, fwd_s.at[e, k], fwd_r.at[e, k], {"ops": peer})

    def place_chunk(e):
        base = base_of(e // halves)
        low = jnp.int32(0)
        for r in range(sectors):
            low = low + (tables[2, r] + tables[3, r] <= base).astype(jnp.int32)
        low = jnp.minimum(low, sectors - overlap)
        source = lax.broadcasted_iota(jnp.int32, (wide, CHUNK), 0)
        target = lax.broadcasted_iota(jnp.int32, (wide, CHUNK), 1)
        for m in range(overlap):
            moved = source + (tables[2, low + m] - base)
            pick[m * wide : (m + 1) * wide, :] = (
                (moved == target) & (source < tables[3, low + m])
            ).astype(jnp.bfloat16)
        found = jnp.concatenate([placed[e % halves, low + m] for m in range(overlap)], axis=1)
        value = jnp.dot(found, pick[...], preferred_element_type=jnp.float32)
        part[e] = value.reshape(outer, 2, share, CHUNK).astype(jnp.bfloat16)
        y_copy(e).start()

    def add_pair(e):
        y_copy(e).wait_recv()
        for k in range(outer - 1):
            dest = lax.rem(row + k + 1, outer)
            sending[e, k] = (
                part[e, dest, side].astype(jnp.float32) + pair_in[e, dest].astype(jnp.float32)
            ).astype(jnp.bfloat16)
            outer_copy(e, k, dest * 2 + side).start()

    def diagonal_of(e):
        cols = cols_of(e)
        h = e % halves
        return (e_share[h] + right_e_ref[0:1, cols]) * psi_share[h, :, cols].astype(jnp.float32)

    def project_diagonal(e):
        diagonal = diagonal_of(e)
        for k in range(vectors):
            product = vec_share[k, e % halves, :, cols_of(e)].astype(jnp.float32) * diagonal
            acc[k] += sum(
                product[r : r + 8, at : at + LANE]
                for r in range(0, share, 8) for at in range(0, CHUNK, LANE)
            )

    def finish(e):
        for k in range(outer - 1):
            outer_copy(e, k, peer).wait_recv()
        total = part[e, row, side].astype(jnp.float32) + pair_in[e, row].astype(jnp.float32)
        for k in range(outer - 1):
            total = total + outer_in[e, k].astype(jnp.float32)
        out_ref[e % halves, me, :, cols_of(e)] = (total + diagonal_of(e)).astype(jnp.bfloat16)
        for k in range(outer - 1):
            gath_copy(e, k, me, lax.rem(row + k + 1, outer) * 2 + side).start()
        fwd_copy(e, outer - 1, me).start()

    def pass_on(e):
        for k in range(outer - 1):
            source = lax.rem(row - k - 1 + outer, outer) * 2 + side
            gath_copy(e, k, source, peer).wait_recv()
            fwd_copy(e, k, source).start()

    local_slots = half_sectors * halves
    slots_all = sectors * halves

    def slot_of(m):
        late = jnp.maximum(m - local_slots, 0)
        early = m < local_slots
        n = jnp.where(early, m % half_sectors, half_sectors + late // halves)
        return n, jnp.where(early, m // half_sectors, late % halves)

    def done(n):
        return jnp.maximum(bond_dim - widest * (sectors - 1 - n), 0) // CHUNK

    def run_stage(stage, m):
        n, h = slot_of(jnp.maximum(m, 0))

        @pl.when((m >= 0) & (m < slots_all) & (done(n) > done(n - 1)))
        def _():
            stage((done(n) - 1) * halves + h)

    stages = ((place_chunk, 0), (add_pair, 1), (finish, 3), (pass_on, 6))

    def slot(m, carry):
        n, h = slot_of(m)

        @pl.when((m >= local_slots) & (h == 0))
        def _():
            remote(
                rbuf.at[n, :, my_half], rbuf.at[n, :, my_half],
                x_s.at[0], x_r.at[n - half_sectors], {"site": across},
            ).wait_recv()
            forward(n, my_half).start()
            forward(n, peer_half).wait_recv()

        apply_sector(n, h)

        @pl.when((m >= local_slots) & (m < local_slots + items))
        def _():
            project_diagonal(m - local_slots)

        for stage, lag in stages:
            run_stage(stage, m - lag)

        return carry

    lax.fori_loop(0, slots_all, slot, 0)

    corr_mine[...] = acc[...]
    corr_copies = []
    for k in range(1, groups):
        copy = remote(
            corr_mine, corr_ops.at[k], ops_s.at[k], ops_r.at[k], {"ops": lax.rem(me + k, groups)}
        )
        copy.start()
        corr_copies.append(copy)
    corr_ops[0] = corr_mine[...]

    def drain(m, carry):
        for stage, lag in stages[1:]:
            run_stage(stage, m - lag)
        return carry

    lax.fori_loop(slots_all, slots_all + 1, drain, 0)

    for copy in corr_copies:
        copy.wait_recv()

    def corr_add(g, total):
        return total + corr_ops[lax.rem(me - g + groups, groups)]

    corr_sites[0] = lax.fori_loop(0, groups, corr_add, jnp.zeros(acc.shape, jnp.float32))
    site_copies = []
    for k in range(1, sites):
        copy = remote(
            corr_sites.at[0], corr_sites.at[k], site_s.at[k], site_r.at[k],
            {"site": lax.rem(here + k, sites)},
        )
        copy.start()
        site_copies.append(copy)

    lax.fori_loop(slots_all + 1, slots_all + 6, drain, 0)

    def last_waits(c, carry):
        fwd_copy(c, outer - 1, peer).wait_recv()
        for k in range(outer - 1):
            source = lax.rem(row - k - 1 + outer, outer) * 2 + 1 - side
            fwd_copy(c, k, source).wait_recv()
        y_copy(c).wait_send()
        for k in range(outer - 1):
            outer_copy(c, k, peer).wait_send()
            gath_copy(c, k, me, peer).wait_send()
            fwd_copy(c, k, me).wait_send()
        fwd_copy(c, outer - 1, me).wait_send()
        return carry

    lax.fori_loop(0, items, last_waits, 0)

    for copy in site_copies:
        copy.wait_recv()

    def site_add(g, total):
        return total + corr_sites[lax.rem(here - g + sites, sites)]

    corr = lax.fori_loop(0, sites, site_add, jnp.zeros(acc.shape, jnp.float32))
    for k in range(vectors):
        corr_out[k] = jnp.sum(corr[k])

    def x_waits(n, carry):
        to_across(n).wait_send()
        forward(n + half_sectors, my_half).wait_send()
        return carry

    lax.fori_loop(0, half_sectors, x_waits, 0)

    def pair_waits(w, carry):
        to_pair(order_of(w)).wait_send()
        return carry

    lax.fori_loop(0, sec_dev, pair_waits, 0)
    for copy in corr_copies + site_copies:
        copy.wait_send()


def local(
    wavefunction,
    left_blocks,
    right_blocks,
    left_sector,
    right_sector,
    term_count,
    left_energy,
    right_energy,
    subspace,
):
    slots, sec_dev, widest = left_blocks.shape[0], left_blocks.shape[1], left_blocks.shape[2]
    bond_dim = wavefunction.shape[0]
    vectors = subspace.shape[0]
    rows = sec_dev * widest
    sites = lax.axis_size("site")
    groups = lax.axis_size("ops")
    sectors = sec_dev * sites
    wide = round_up(widest, 256)
    window = round_up(widest + LANE - 1, LANE)
    outer = groups // 2
    halves = 2 if groups > 99 and rows // 2 % (16 * groups) == 0 and sec_dev % 2 == 0 else 1
    rows = rows // halves
    share = rows // groups
    items = bond_dim // CHUNK * halves
    tiles = bond_dim // LANE
    half_sectors = sectors // 2
    outside = -(-(bond_dim - CHUNK - 2 * (widest - 1)) // widest)
    overlap = min(sectors, sectors - outside)

    assert sites == 4 and slots % 4 == 0 and 2 * (wide - widest) == LANE and wide == 2 * LANE

    labels = jnp.arange(sectors, dtype=jnp.int32)
    ids = jnp.stack([left_sector, right_sector])
    starts = jnp.sum((ids[:, None, :] < labels[None, :, None]).astype(jnp.int32), axis=2)
    sizes = jnp.sum((ids[:, None, :] == labels[None, :, None]).astype(jnp.int32), axis=2)
    tables = jnp.stack([starts, sizes], axis=1).reshape(4, sectors)

    vmem = pl.BlockSpec(memory_space=pltpu.VMEM)
    smem = pl.BlockSpec(memory_space=pltpu.SMEM)
    hbm = pl.BlockSpec(memory_space=pl.ANY)
    dma = pltpu.SemaphoreType.DMA
    bf16, f32 = jnp.bfloat16, jnp.float32
    sigma, corr = pl.pallas_call(
        functools.partial(step_kernel, groups, sites),
        out_shape=(
            jax.ShapeDtypeStruct((halves, groups, share, bond_dim), bf16),
            jax.ShapeDtypeStruct((vectors,), f32),
        ),
        in_specs=[smem, smem, hbm, hbm, hbm, hbm, hbm, vmem, vmem],
        out_specs=(vmem, smem),
        scratch_shapes=[
            pltpu.VMEM((slots // 2, 2, sec_dev, widest, widest), bf16),
            pltpu.VMEM((slots, sec_dev, widest, widest), bf16),
            pltpu.VMEM((tiles, LANE, bond_dim), bf16),
            pltpu.VMEM((vectors, halves, tiles, rows, LANE), bf16),
            pltpu.VMEM((vectors, halves, share, bond_dim), bf16),
            pltpu.VMEM((halves, tiles, rows, LANE), bf16),
            pltpu.VMEM((halves, share, bond_dim), bf16),
            pltpu.VMEM((halves, share, 1), f32),
            pltpu.VMEM((sectors, widest, slots * widest), bf16),
            pltpu.VMEM((wide, slots * widest), bf16),
            pltpu.VMEM((2, rows, wide), bf16),
            pltpu.VMEM((rows, slots * widest), bf16),
            pltpu.VMEM((rows, wide), f32),
            pltpu.VMEM((vectors, rows, wide), bf16),
            pltpu.VMEM((halves, sectors, rows, wide), bf16),
            pltpu.VMEM((overlap * wide, CHUNK), bf16),
            pltpu.VMEM((items, outer, 2, share, CHUNK), bf16),
            pltpu.VMEM((items, outer, share, CHUNK), bf16),
            pltpu.VMEM((items, outer - 1, share, CHUNK), bf16),
            pltpu.VMEM((items, outer - 1, share, CHUNK), bf16),
            pltpu.VMEM((vectors, 8, LANE), f32),
            pltpu.VMEM((vectors, 8, LANE), f32),
            pltpu.VMEM((groups, vectors, 8, LANE), f32),
            pltpu.VMEM((sites, vectors, 8, LANE), f32),
            dma((4 + vectors * halves * tiles,)),
            dma((half_sectors,)), dma((half_sectors,)),
            dma((half_sectors,)), dma((half_sectors,)),
            dma((half_sectors,)), dma((half_sectors,)),
            dma((items,)), dma((items,)),
            dma((items, outer)), dma((items, outer)),
            dma((items, outer)), dma((items, outer)),
            dma((items, outer)), dma((items, outer)),
            dma((groups,)), dma((groups,)),
            dma((sites,)), dma((sites,)),
        ],
        compiler_params=pltpu.CompilerParams(
            collective_id=0, has_side_effects=True, vmem_limit_bytes=66_900_000
        ),
        name="davidson_step",
    )(
        tables,
        term_count,
        left_blocks.reshape(slots // 2, 2, sec_dev, widest, widest),
        right_blocks,
        wavefunction.reshape(tiles, LANE, bond_dim),
        subspace.reshape(vectors, halves, rows, bond_dim),
        subspace.reshape(vectors, halves, groups, share, bond_dim),
        left_energy.reshape(tiles, 1, LANE),
        right_energy[None, :],
    )
    return (sigma.reshape(sec_dev, widest, bond_dim), corr)


def solution(mesh):
    in_specs = (
        P(),
        P("ops", "site", None, None),
        P("ops", "site", None, None),
        P(),
        P(),
        P("ops"),
        P(),
        P(),
        P(None, "site", None, None),
    )
    out_specs = (P("site", None, None), P())
    return jax.shard_map(local, mesh=mesh, in_specs=in_specs, out_specs=out_specs, check_vma=False)
```
